128 devices in a mesh: row: 8 (over z, x_lo), col: 16 (over y, x_hi, core).
Axes of the slice: x: 4 (x_hi: 2, x_lo: 2; x = x_hi * 2 + x_lo), y: 4, z: 4, core: 2. Of those that a mesh axis runs over, the one named last changes fastest.
Arguments:
- normal_matrix: float32 [14336, 14336], P(('row', 'col')), may hold values from -90 to 90, as said below
- new_index: int32 [14336], replicated, may hold values from 0 to 14335, each once
- check_vectors: float32 [14336, 1024], P('col'), may hold values from -0.046875 to 0.046875
Outputs:
- tile_layout: float32 [14336, 14336], P('row', 'col')
- check_product: float32 [14336, 1024], P(('row', 'col'))
The draws below stay inside these ranges and needn't reach their ends.
Inputs may be any that keep to these rules, and one draw needn't show every extreme that they name: normal_matrix is symmetric. new_index[a] is the new index of parameter a; every index 0 to 14335 appears once.
All inputs are finite; a program needn't handle non-finite values.
Results may differ from the reference program's by a relative error of at most 0.000082.
Values sent between devices are 32-bit elements; how exact they have to be, the bound alone decides.
No kernel may reach another device: no remote copies, remote signals or barrier semaphores. Data moves between devices by JAX's collectives and lax.ppermute only.
A program may use at most 128 MiB of HBM per device.

```python
import jax
import jax.numpy as jnp
from jax import lax

NPAR = 14336
TILE = 128
VECTORS = 1024
N_ROW = 8
N_COL = 16


def draw_normal_matrix(key, part):
    key_entries = jax.random.fold_in(key, 11)
    key_diagonal = jax.random.fold_in(key, 12)
    entries = jnp.clip(jax.random.normal(key_entries, (NPAR, NPAR), jnp.float32), -6.0, 6.0)
    symmetric = (entries + entries.T) * 0.7071
    diagonal_lift = jax.random.uniform(key_diagonal, (NPAR,), jnp.float32, 2.0, 8.0)
    return symmetric + jnp.diag(diagonal_lift)


def shard_levels(key, extent, split, smallest, largest):
    def one(dim, shards_of):
        steps = jax.random.uniform(jax.random.fold_in(jax.random.fold_in(key, 6), dim), (shards_of,), jnp.float32, smallest / len(split), largest / len(split))
        return jnp.repeat(jnp.exp(steps), extent[dim] // shards_of).reshape((-1,) + (1,) * (len(extent) - dim - 1))

    level = one(*split[0])
    for cut in split[1:]:
        level = level * one(*cut)
    return level


def scatter_about(own_key, extent, spread, most, pieces=(), kind=jnp.bfloat16):
    factor_of = shard_levels(own_key, extent, pieces, -0.22, 0.18) if pieces else 1.0
    array = jax.random.normal(own_key, extent, jnp.float32) * spread * factor_of
    return jnp.minimum(jnp.maximum(array, -most), most).astype(kind)


def setup_inputs(seed: int = 0) -> dict:
    key_list = jax.random.split(jax.random.key(seed), 4)
    return {
        "normal_matrix": draw_normal_matrix(jax.random.fold_in(key_list[3], 71), 0),
        "new_index": jax.random.permutation(key_list[1], NPAR).astype(jnp.int32),
        "check_vectors": scatter_about(key_list[2], (NPAR, VECTORS), NPAR ** -0.5, 0.046875, ((0, 16),), jnp.float32),
    }


def new_of_packed(places, groups, stride, tile_size):
    holder = places // stride
    within = places % stride
    return ((within // tile_size) * groups + holder) * tile_size + within % tile_size


def reference(normal_matrix, new_index, check_vectors):
    places = jnp.arange(NPAR, dtype=jnp.int32)
    old_of_new = jnp.zeros((NPAR,), jnp.int32).at[new_index].set(places)
    row_pick = old_of_new[new_of_packed(places, N_ROW, NPAR // N_ROW, TILE)]
    col_pick = old_of_new[new_of_packed(places, N_COL, NPAR // N_COL, TILE)]
    tile_layout = jnp.take(jnp.take(normal_matrix, row_pick, axis=0), col_pick, axis=1)
    check_product = jnp.dot(tile_layout, check_vectors, precision=lax.Precision.HIGHEST, preferred_element_type=jnp.float32)
    return tile_layout, check_product
```

```python
import jax
import jax.numpy as jnp
from jax import lax
from jax.experimental import pallas as pl
from jax.experimental.pallas import tpu as pltpu
from jax.sharding import PartitionSpec as P

TILE = 128
LANES = 128
VMEM = 56 * 1024 * 1024


def scatter_rows(pos_ref, base, src_ref, dst_ref, count, unroll=32):
    def body(i, carry):
        start = i * unroll
        for u in range(unroll):
            dst_ref[pl.ds(pos_ref[base + start + u], 1), :] = src_ref[pl.ds(start + u, 1), :]
        return carry

    lax.fori_loop(0, count // unroll, body, 0)


def group_columns(slab, places, devices):
    share, unknowns = slab.shape
    width = 1024
    steps = unknowns // width
    keep = share - 8
    chunk = LANES - share

    def kernel(pos_ref, x_ref, out_ref, turned, spread):
        step = pl.program_id(0)
        for b in range(width // LANES):
            turned[b * LANES:(b + 1) * LANES, :share] = x_ref[:, b * LANES:(b + 1) * LANES].T
        scatter_rows(pos_ref, step * width, turned, spread, width)

        @pl.when(step == steps - 1)
        def _():
            def pack(d, carry):
                out_ref[d] = spread[pl.ds(pl.multiple_of(d * keep, 8), keep), :]
                extra = spread[pl.ds(pl.multiple_of(devices * keep + d * 8, 8), 8), :]
                for k in range(share // chunk):
                    out_ref[d, 8 * k:8 * k + 8, share:] = extra[:, chunk * k:chunk * (k + 1)]
                return carry

            lax.fori_loop(0, devices, pack, 0)

    return pl.pallas_call(
        kernel,
        grid_spec=pltpu.PrefetchScalarGridSpec(
            num_scalar_prefetch=1,
            grid=(steps,),
            in_specs=[pl.BlockSpec((share, width), lambda g, pos: (0, g))],
            out_specs=pl.BlockSpec((devices, keep, LANES), lambda g, pos: (0, 0, 0)),
            scratch_shapes=[
                pltpu.VMEM((width, LANES), jnp.float32),
                pltpu.VMEM((unknowns, LANES), jnp.float32),
            ],
        ),
        out_shape=jax.ShapeDtypeStruct((devices, keep, LANES), jnp.float32),
        compiler_params=pltpu.CompilerParams(vmem_limit_bytes=VMEM),
        name="group_columns",
    )(places, slab)


def group_rows(blocks, places, groups, share):
    devices, keep, _ = blocks.shape
    unknowns = devices * share
    chunk = LANES - share
    per = 8
    steps = devices // per
    rows = unknowns // groups

    def kernel(pos_ref, x_ref, out_ref, turned, spread):
        step = pl.program_id(0)
        for b in range(per):
            flipped = x_ref[b].T
            turned[b * share:(b + 1) * share, :keep] = flipped[:share]
            for k in range(share // chunk):
                turned[b * share + k * chunk:b * share + (k + 1) * chunk, keep:share] = flipped[share:, 8 * k:8 * k + 8]
        scatter_rows(pos_ref, step * per * share, turned, spread, per * share)

        @pl.when(step == steps - 1)
        def _():
            def turn(g, carry):
                for k in range(rows // LANES):
                    piece = spread[pl.ds(pl.multiple_of(g * rows + k * LANES, LANES), LANES), :]
                    out_ref[g, :, k * LANES:(k + 1) * LANES] = piece.T[:share]
                return carry

            lax.fori_loop(0, groups, turn, 0)

    return pl.pallas_call(
        kernel,
        grid_spec=pltpu.PrefetchScalarGridSpec(
            num_scalar_prefetch=1,
            grid=(steps,),
            in_specs=[pl.BlockSpec((per, keep, LANES), lambda g, pos: (g, 0, 0))],
            out_specs=pl.BlockSpec((groups, share, rows), lambda g, pos: (0, 0, 0)),
            scratch_shapes=[
                pltpu.VMEM((per * share, LANES), jnp.float32),
                pltpu.VMEM((unknowns, LANES), jnp.float32),
            ],
        ),
        out_shape=jax.ShapeDtypeStruct((groups, share, rows), jnp.float32),
        compiler_params=pltpu.CompilerParams(vmem_limit_bytes=VMEM),
        name="group_rows",
    )(places, blocks)


def tile_and_product(turned, vectors, core, share):
    columns, rows = turned.shape
    width = vectors.shape[1]
    high = 256 if rows % 256 == 0 else 128
    pairs = rows // (2 * share)

    def split(x):
        hi = x.astype(jnp.bfloat16)
        return hi, (x - hi.astype(jnp.float32)).astype(jnp.bfloat16)

    def kernel(core_ref, x_ref, v_ref, tile_ref, other_ref, mine_ref, v_hi, v_lo):
        step = pl.program_id(0)

        @pl.when(step == 0)
        def _():
            v_hi[...], v_lo[...] = split(v_ref[...])
            for k in range(rows // LANES):
                tile_ref[k * LANES:(k + 1) * LANES, :] = x_ref[:, k * LANES:(k + 1) * LANES].T

        x = tile_ref[pl.ds(pl.multiple_of(step * 2 * share, 8), 2 * share), :]
        hi, lo = split(x)
        part = (
            jnp.dot(hi, v_hi[...], preferred_element_type=jnp.float32)
            + jnp.dot(hi, v_lo[...], preferred_element_type=jnp.float32)
            + jnp.dot(lo, v_hi[...], preferred_element_type=jnp.float32)
        )
        first, second = part[:share], part[share:]
        even = core_ref[0] == 0
        other_ref[0] = jnp.where(even, second, first)
        mine_ref[0] = jnp.where(even, first, second)

    half = jax.ShapeDtypeStruct((pairs, share, width), jnp.float32)
    half_spec = pl.BlockSpec((1, share, width), lambda g, core: (g, 0, 0))
    return pl.pallas_call(
        kernel,
        grid_spec=pltpu.PrefetchScalarGridSpec(
            num_scalar_prefetch=1,
            grid=(pairs,),
            in_specs=[
                pl.BlockSpec((columns, rows), lambda g, core: (0, 0)),
                pl.BlockSpec((columns, width), lambda g, core: (0, 0)),
            ],
            out_specs=[pl.BlockSpec((rows, columns), lambda g, core: (0, 0)), half_spec, half_spec],
            scratch_shapes=[
                pltpu.VMEM((columns, width), jnp.bfloat16),
                pltpu.VMEM((columns, width), jnp.bfloat16),
            ],
        ),
        out_shape=[jax.ShapeDtypeStruct((rows, columns), jnp.float32), half, half],
        compiler_params=pltpu.CompilerParams(vmem_limit_bytes=VMEM),
        name="tile_and_product",
    )(core, turned, vectors)


def shards(normal_matrix, new_index, check_vectors):
    row_count = lax.axis_size("row")
    col_count = lax.axis_size("col")
    devices = row_count * col_count
    share, unknowns = normal_matrix.shape
    keep = share - 8

    tile, lane = new_index // TILE, new_index % TILE
    within_col = tile // col_count * TILE + lane
    block = within_col // share * col_count + tile % col_count
    place = within_col % share
    column_places = jnp.where(
        place < keep, block * keep + place, devices * keep + block * 8 + place - keep
    )
    row_places = tile % row_count * (unknowns // row_count) + tile // row_count * TILE + lane

    outgoing = group_columns(normal_matrix, column_places, devices)
    arrived = lax.all_to_all(outgoing, ("row", "col"), split_axis=0, concat_axis=0, tiled=True)
    chosen = group_rows(arrived, row_places, row_count, share)
    moved = lax.all_to_all(chosen, "row", split_axis=0, concat_axis=0, tiled=True)
    turned = moved.reshape(row_count * share, unknowns // row_count)

    me = lax.axis_index("col")
    core = (me % 2).astype(jnp.int32).reshape(1)
    tile_layout, other, mine = tile_and_product(turned, check_vectors, core, share)
    swap = [(i, i ^ 1) for i in range(col_count)]
    both = mine + lax.ppermute(other, "col", swap)
    groups = [list(range(p, col_count, 2)) for p in range(2)]
    parts = lax.all_to_all(both, "col", split_axis=0, concat_axis=0, axis_index_groups=groups, tiled=True)
    return tile_layout, parts.sum(axis=0)


def solution(mesh):
    return jax.shard_map(
        shards,
        mesh=mesh,
        in_specs=(P(("row", "col"), None), P(), P("col", None)),
        out_specs=(P("row", "col"), P(("row", "col"), None)),
        check_vma=False,
    )
```

```python
import jax
import jax.numpy as jnp
from jax import lax
from jax.experimental import pallas as pl
from jax.experimental.pallas import tpu as pltpu
from jax.sharding import PartitionSpec as P

TILE = 128
LANES = 128
SUB = 8
VMEM = 56 * 1024 * 1024


def scatter_rows(pos_ref, base, src_ref, dst_ref, count, unroll=32):
    def body(i, carry):
        start = i * unroll
        for u in range(unroll):
            dst_ref[pl.ds(pos_ref[base + start + u], 1), :] = src_ref[pl.ds(start + u, 1), :]
        return carry

    lax.fori_loop(0, count // unroll, body, 0)


def params(**kwargs):
    return pltpu.CompilerParams(vmem_limit_bytes=VMEM, **kwargs)


def group_columns(slab, places, devices, full, rest):
    share, unknowns = slab.shape
    steps = 4
    width = unknowns // steps
    keep = full - SUB
    chunk = LANES - share
    outs = 4
    per = devices // outs
    second = devices * keep
    extra_at = second + devices * rest

    def kernel(pos_ref, x_ref, full_ref, rest_ref, turned, spread):
        step = pl.program_id(0)

        @pl.when(step < steps)
        def _():
            for b in range(width // LANES):
                turned[b * LANES:(b + 1) * LANES, :share] = x_ref[:, b * LANES:(b + 1) * LANES].T
            scatter_rows(pos_ref, step * width, turned, spread, width)

        @pl.when(step >= steps)
        def _():
            first = (step - steps) * per

            def pack(i, carry):
                for u in range(8):
                    b = i * 8 + u
                    d = first + b
                    full_ref[b] = spread[pl.ds(pl.multiple_of(d * keep, SUB), keep), :]
                    rest_ref[b] = spread[pl.ds(pl.multiple_of(second + d * rest, SUB), rest), :]
                    extra = spread[pl.ds(pl.multiple_of(extra_at + d * SUB, SUB), SUB), :]
                    for k in range(share // chunk):
                        full_ref[b, SUB * k:SUB * k + SUB, share:] = extra[:, chunk * k:chunk * (k + 1)]
                return carry

            lax.fori_loop(0, per // 8, pack, 0)

    late = lambda g, pos: (jnp.maximum(g - steps, 0), 0, 0)
    return pl.pallas_call(
        kernel,
        grid_spec=pltpu.PrefetchScalarGridSpec(
            num_scalar_prefetch=1,
            grid=(steps + outs,),
            in_specs=[pl.BlockSpec((share, width), lambda g, pos: (0, jnp.minimum(g, steps - 1)))],
            out_specs=[
                pl.BlockSpec((per, keep, LANES), late),
                pl.BlockSpec((per, rest, LANES), late),
            ],
            scratch_shapes=[
                pltpu.VMEM((width, LANES), jnp.float32),
                pltpu.VMEM((unknowns, LANES), jnp.float32),
            ],
        ),
        out_shape=[
            jax.ShapeDtypeStruct((devices, keep, LANES), jnp.float32),
            jax.ShapeDtypeStruct((devices, rest, LANES), jnp.float32),
        ],
        compiler_params=params(),
        name="group_columns",
    )(places, slab)


def group_rows(blocks, places, groups, share, packed, widths, label):
    devices, held, _ = blocks.shape
    count = held + SUB if packed else held
    unknowns = devices * share
    chunk = LANES - share
    steps = 4
    per = devices // steps
    rows = unknowns // groups
    starts = [sum(widths[:i]) for i in range(len(widths))]
    outs = groups

    def kernel(pos_ref, x_ref, *refs):
        out_refs, (turned, spread) = refs[:-2], refs[-2:]
        step = pl.program_id(0)

        @pl.when(step < steps)
        def _():
            def flip(i, carry):
                for u in range(4):
                    b = i * 4 + u
                    flipped = x_ref[b].T
                    at = pl.multiple_of(b * share, SUB)
                    turned[pl.ds(at, share), :held] = flipped[:share]
                    if packed:
                        for k in range(share // chunk):
                            turned[pl.ds(at + k * chunk, chunk), held:count] = flipped[share:, SUB * k:SUB * k + SUB]
                return carry

            lax.fori_loop(0, per // 4, flip, 0)
            scatter_rows(pos_ref, step * per * share, turned, spread, per * share)

        @pl.when(step >= steps)
        def _():
            g = step - steps
            for ref, start, width in zip(out_refs, starts, widths):
                for k in range(width // LANES):
                    at = pl.multiple_of(g * rows + start + k * LANES, LANES)
                    ref[0, :, k * LANES:(k + 1) * LANES] = spread[pl.ds(at, LANES), :].T[:count]

    late = lambda g, pos: (jnp.maximum(g - steps, 0), 0, 0)
    return pl.pallas_call(
        kernel,
        grid_spec=pltpu.PrefetchScalarGridSpec(
            num_scalar_prefetch=1,
            grid=(steps + outs,),
            in_specs=[pl.BlockSpec((per, held, LANES), lambda g, pos: (jnp.minimum(g, steps - 1), 0, 0))],
            out_specs=[pl.BlockSpec((1, count, w), late) for w in widths],
            scratch_shapes=[
                pltpu.VMEM((per * share, LANES), jnp.float32),
                pltpu.VMEM((unknowns, LANES), jnp.float32),
            ],
        ),
        out_shape=[jax.ShapeDtypeStruct((groups, count, w), jnp.float32) for w in widths],
        compiler_params=params(),
        cost_estimate=pl.CostEstimate(flops=20_000_000_000, bytes_accessed=2 * unknowns * count * 4, transcendentals=0),
        name=label,
    )(places, blocks)


def tile_and_product(pieces, v_hi, v_lo, core, tile, cols, share, index, label):
    groups, _, rows = pieces[0].shape
    counts = [p.shape[1] for p in pieces]
    span = rows // cols
    columns, width = v_hi.shape
    steps = 4
    wide = width // steps

    def kernel(core_ref, *refs):
        x_refs = refs[:len(pieces)]
        hi_ref, lo_ref = refs[len(pieces):len(pieces) + 2]
        tile_ref, other_ref, mine_ref, x_hi, x_lo = refs[-5:]
        step = pl.program_id(0)

        @pl.when(step == 0)
        def _():
            for k in range(rows // LANES):
                held = []
                for g in range(groups):
                    for x_ref in x_refs:
                        held.append(x_ref[g, :, k * LANES:(k + 1) * LANES])
                x = jnp.concatenate(held, axis=0).T
                hi = x.astype(jnp.bfloat16)
                x_hi[k * LANES:(k + 1) * LANES, :] = hi
                x_lo[k * LANES:(k + 1) * LANES, :] = (x - hi.astype(jnp.float32)).astype(jnp.bfloat16)
                for s in range(0, LANES, SUB):
                    c, m = divmod(k * LANES + s, span)
                    tile_ref[c, m:m + SUB, :] = x[s:s + SUB]

        part = (
            jnp.dot(x_hi[...], hi_ref[...], preferred_element_type=jnp.float32)
            + jnp.dot(x_hi[...], lo_ref[...], preferred_element_type=jnp.float32)
            + jnp.dot(x_lo[...], hi_ref[...], preferred_element_type=jnp.float32)
        )
        even = core_ref[0] == 0
        for c in range(cols // 2):
            first = part[2 * c * span:(2 * c + 1) * span]
            second = part[(2 * c + 1) * span:(2 * c + 2) * span]
            other_ref[c] = jnp.where(even, second, first)
            mine_ref[c] = jnp.where(even, first, second)

    half = jax.ShapeDtypeStruct((cols // 2, span, width), jnp.float32)
    half_spec = pl.BlockSpec((cols // 2, span, wide), lambda g, core: (0, 0, g))
    in_specs = [pl.BlockSpec((groups, n, rows), lambda g, core: (0, 0, 0)) for n in counts]
    in_specs += [pl.BlockSpec((columns, wide), lambda g, core: (0, g))] * 2
    operands = [core, *pieces, v_hi, v_lo]
    aliases = {}
    if tile is not None:
        aliases = {len(operands): 0}
        operands.append(tile)
        in_specs.append(pl.BlockSpec(memory_space=pl.ANY))
    return pl.pallas_call(
        kernel,
        grid_spec=pltpu.PrefetchScalarGridSpec(
            num_scalar_prefetch=1,
            grid=(steps,),
            in_specs=in_specs,
            out_specs=[pl.BlockSpec((cols, span, columns), lambda g, core: (0, index, 0)), half_spec, half_spec],
            scratch_shapes=[
                pltpu.VMEM((rows, columns), jnp.bfloat16),
                pltpu.VMEM((rows, columns), jnp.bfloat16),
            ],
        ),
        out_shape=[jax.ShapeDtypeStruct((cols, share, columns), jnp.float32), half, half],
        input_output_aliases=aliases,
        compiler_params=params(),
        cost_estimate=pl.CostEstimate(flops=6 * rows * columns * width, bytes_accessed=8 * rows * columns, transcendentals=0),
        name=label,
    )(*operands)


def shards(normal_matrix, new_index, check_vectors):
    row_count = lax.axis_size("row")
    col_count = lax.axis_size("col")
    devices = row_count * col_count
    share, unknowns = normal_matrix.shape
    full, rest = 64, 48
    spans = (56, 56)
    keep = full - SUB
    rows = unknowns // row_count

    tile, lane = new_index // TILE, new_index % TILE
    within_col = tile // col_count * TILE + lane
    block = within_col // share * col_count + tile % col_count
    place = within_col % share
    column_places = jnp.where(
        place < keep,
        block * keep + place,
        jnp.where(
            place < full,
            devices * (keep + rest) + block * SUB + place - keep,
            devices * keep + block * rest + place - full,
        ),
    )
    within_row = tile // row_count * TILE + lane
    owner, m = within_row // share, within_row % share
    spot = jnp.zeros_like(m)
    start = 0
    for span in spans:
        spot = jnp.where((m >= start) & (m < start + span), start * col_count + owner * span + m - start, spot)
        start += span
    row_places = tile % row_count * rows + spot

    exchange = lambda x: lax.all_to_all(x, ("row", "col"), split_axis=0, concat_axis=0, tiled=True)
    along = lambda x: lax.all_to_all(x, "row", split_axis=0, concat_axis=0, tiled=True)
    groups = [list(range(p, col_count, 2)) for p in range(2)]
    swap = [(i, i ^ 1) for i in range(col_count)]
    widths = [s * col_count for s in spans]

    out_full, out_rest = group_columns(normal_matrix, column_places, devices, full, rest)
    in_full = exchange(out_full)
    out_rest, in_full = lax.optimization_barrier((out_rest, in_full))
    in_rest = exchange(out_rest)
    v_hi = lax.reduce_precision(check_vectors, 8, 7)
    v_lo = (check_vectors - v_hi).astype(jnp.bfloat16)
    v_hi = v_hi.astype(jnp.bfloat16)
    core = (lax.axis_index("col") % 2).astype(jnp.int32).reshape(1)

    chosen_full = group_rows(in_full, row_places, row_count, share, True, widths, "group_rows_full")
    chosen_rest = group_rows(in_rest, row_places, row_count, share, False, widths, "group_rows_rest")

    tile_layout = None
    sums = []
    last = in_rest
    for q, span in enumerate(spans):
        pieces = []
        for chosen in (chosen_full, chosen_rest):
            send, _ = lax.optimization_barrier((chosen[q], last))
            last = along(send)
            pieces.append(last)
        tile_layout, other, mine = tile_and_product(
            pieces, v_hi, v_lo, core, tile_layout, col_count, share, q, f"tile_and_product_{q}"
        )
        both = mine + lax.ppermute(other, "col", swap)
        parts = lax.all_to_all(both, "col", split_axis=0, concat_axis=0, axis_index_groups=groups, tiled=True)
        sums.append(parts.sum(axis=0))
    return tile_layout.reshape(rows, unknowns // col_count), jnp.concatenate(sums, axis=0)


def solution(mesh):
    return jax.shard_map(
        shards,
        mesh=mesh,
        in_specs=(P(("row", "col"), None), P(), P("col", None)),
        out_specs=(P("row", "col"), P(("row", "col"), None)),
        check_vma=False,
    )
```

```python
import jax
import jax.numpy as jnp
from jax import lax
from jax.experimental import pallas as pl
from jax.experimental.pallas import tpu as pltpu
from jax.sharding import PartitionSpec as P


TILE = 128
LANES = 128
SUB = 8
VMEM = 56 * 1024 * 1024
UNROLL = 32
SPANS = (56, 56)


def params():
    return pltpu.CompilerParams(vmem_limit_bytes=VMEM)


def group_columns(slab, places, devices):
    share, unknowns = slab.shape
    steps, _, width = places.shape
    keep = share - SUB
    chunk = LANES - share
    outs = 4
    per = devices // outs

    def kernel(pos_ref, x_ref, out_ref, turned, spread):
        step = pl.program_id(0)

        @pl.when(step < steps)
        def _():
            for b in range(width // LANES):
                turned[b * LANES:(b + 1) * LANES, :share] = x_ref[:, b * LANES:(b + 1) * LANES].T

            def scatter(i, carry):
                start = i * UNROLL
                for u in range(UNROLL):
                    spread[pl.ds(pos_ref[0, 0, start + u], 1), :] = turned[pl.ds(start + u, 1), :]
                return carry

            lax.fori_loop(0, width // UNROLL, scatter, 0)

        @pl.when(step >= steps)
        def _():
            first = (step - steps) * per

            def pack(i, carry):
                for u in range(8):
                    b = i * 8 + u
                    x = spread[pl.ds(pl.multiple_of((first + b) * share, SUB), share), :].T
                    out_ref[b, :, :share] = x[:keep]
                    for k in range(share // chunk):
                        out_ref[b, SUB * k:SUB * k + SUB, share:] = x[keep:share, chunk * k:chunk * (k + 1)]
                return carry

            lax.fori_loop(0, per // 8, pack, 0)

    return pl.pallas_call(
        kernel,
        grid=(steps + outs,),
        in_specs=[
            pl.BlockSpec((1, 1, width), lambda g: (jnp.minimum(g, steps - 1), 0, 0), memory_space=pltpu.SMEM),
            pl.BlockSpec((share, width), lambda g: (0, jnp.minimum(g, steps - 1))),
        ],
        out_specs=pl.BlockSpec((per, keep, LANES), lambda g: (jnp.maximum(g - steps, 0), 0, 0)),
        scratch_shapes=[
            pltpu.VMEM((width, LANES), jnp.float32),
            pltpu.VMEM((unknowns, LANES), jnp.float32),
        ],
        out_shape=jax.ShapeDtypeStruct((devices, keep, LANES), jnp.float32),
        compiler_params=params(),
        name="group_columns",
    )(places, slab)


def group_rows(blocks, places, groups, share, widths):
    devices, keep, _ = blocks.shape
    unknowns = devices * share
    chunk = LANES - share
    steps = places.shape[0]
    per = devices // steps
    rows = unknowns // groups
    starts = [sum(widths[:i]) for i in range(len(widths))]
    outs = 4
    each = groups // outs

    def kernel(pos_ref, x_ref, *refs):
        out_refs, (extra, spread) = refs[:-2], refs[-2:]
        step = pl.program_id(0)

        @pl.when(step < steps)
        def _():
            def unpack(i, carry):
                for u in range(8):
                    b = i * 8 + u
                    at = pl.multiple_of(b * SUB, SUB)
                    for k in range(share // chunk):
                        extra[pl.ds(at, SUB), chunk * k:chunk * (k + 1)] = x_ref[b, SUB * k:SUB * k + SUB, share:]
                return carry

            lax.fori_loop(0, per // 8, unpack, 0)

            def scatter(b, carry):
                start = b * share
                for u in range(keep):
                    spread[pl.ds(pos_ref[0, 0, start + u], 1), :] = x_ref[b, pl.ds(u, 1), :]
                for u in range(SUB):
                    spread[pl.ds(pos_ref[0, 0, start + keep + u], 1), :] = extra[pl.ds(b * SUB + u, 1), :]
                return carry

            lax.fori_loop(0, per, scatter, 0)

        @pl.when(step >= steps)
        def _():
            def turn(e, carry):
                g = (step - steps) * each + e
                for ref, start, width in zip(out_refs, starts, widths):
                    for k in range(width // LANES):
                        at = pl.multiple_of(g * rows + start + k * LANES, LANES)
                        ref[e, :, k * LANES:(k + 1) * LANES] = spread[pl.ds(at, LANES), :].T[:share]
                return carry

            lax.fori_loop(0, each, turn, 0)

    late = lambda g: (jnp.maximum(g - steps, 0), 0, 0)
    early = lambda g: (jnp.minimum(g, steps - 1), 0, 0)
    return pl.pallas_call(
        kernel,
        grid=(steps + outs,),
        in_specs=[
            pl.BlockSpec((1, 1, per * share), early, memory_space=pltpu.SMEM),
            pl.BlockSpec((per, keep, LANES), early),
        ],
        out_specs=[pl.BlockSpec((each, share, w), late) for w in widths],
        scratch_shapes=[
            pltpu.VMEM((per * SUB, LANES), jnp.float32),
            pltpu.VMEM((unknowns, LANES), jnp.float32),
        ],
        out_shape=[jax.ShapeDtypeStruct((groups, share, w), jnp.float32) for w in widths],
        compiler_params=params(),
        name="group_rows",
    )(places, blocks)


def tile_and_product(turned, v_hi, v_lo, where, tile, cols, share, offset):
    groups, _, rows = turned.shape
    span = rows // cols
    columns, width = v_hi.shape
    steps = 4
    wide = width // steps
    pairs = cols // 2

    def kernel(where_ref, x_ref, hi_ref, lo_ref, *refs):
        tile_ref, other_ref, mine_ref, x_hi, x_lo, held, sem = refs[-7:]
        step = pl.program_id(0)
        store = pltpu.make_async_copy(held, tile_ref.at[:, offset:offset + span, :], sem)

        @pl.when(step == 0)
        def _():
            for k in range(rows // LANES):
                x = x_ref[:, :, k * LANES:(k + 1) * LANES].reshape(columns, LANES).T
                hi = x.astype(jnp.bfloat16)
                x_hi[k * LANES:(k + 1) * LANES, :] = hi
                x_lo[k * LANES:(k + 1) * LANES, :] = (x - hi.astype(jnp.float32)).astype(jnp.bfloat16)
                for s in range(0, LANES, SUB):
                    c, m = divmod(k * LANES + s, span)
                    held[c, m:m + SUB, :] = x[s:s + SUB]
            store.start()

        part = (
            jnp.dot(x_hi[...], hi_ref[...], preferred_element_type=jnp.float32)
            + jnp.dot(x_hi[...], lo_ref[...], preferred_element_type=jnp.float32)
            + jnp.dot(x_lo[...], hi_ref[...], preferred_element_type=jnp.float32)
        )
        even = where_ref[0] == 0
        for c in range(pairs):
            slot = c ^ where_ref[1]
            first = part[2 * c * span:(2 * c + 1) * span]
            second = part[(2 * c + 1) * span:(2 * c + 2) * span]
            other_ref[slot] = jnp.where(even, second, first)
            mine_ref[slot] = jnp.where(even, first, second)

        @pl.when(step == steps - 1)
        def _():
            store.wait()

    half = jax.ShapeDtypeStruct((pairs, span, width), jnp.float32)
    half_spec = pl.BlockSpec((pairs, span, wide), lambda g, where: (0, 0, g))
    in_specs = [pl.BlockSpec((groups, share, rows), lambda g, where: (0, 0, 0))]
    in_specs += [pl.BlockSpec((columns, wide), lambda g, where: (0, g))] * 2
    operands = [where, turned, v_hi, v_lo]
    aliases = {}
    if tile is not None:
        aliases = {len(operands): 0}
        operands.append(tile)
        in_specs.append(pl.BlockSpec(memory_space=pl.ANY))
    return pl.pallas_call(
        kernel,
        grid_spec=pltpu.PrefetchScalarGridSpec(
            num_scalar_prefetch=1,
            grid=(steps,),
            in_specs=in_specs,
            out_specs=[pl.BlockSpec(memory_space=pl.ANY), half_spec, half_spec],
            scratch_shapes=[
                pltpu.VMEM((rows, columns), jnp.bfloat16),
                pltpu.VMEM((rows, columns), jnp.bfloat16),
                pltpu.VMEM((cols, span, columns), jnp.float32),
                pltpu.SemaphoreType.DMA,
            ],
        ),
        out_shape=[jax.ShapeDtypeStruct((cols, share, columns), jnp.float32), half, half],
        input_output_aliases=aliases,
        compiler_params=params(),
        cost_estimate=pl.CostEstimate(flops=6 * rows * columns * width, bytes_accessed=8 * rows * columns, transcendentals=0),
    )(*operands)


def shards(normal_matrix, new_index, check_vectors):
    row_count = lax.axis_size("row")
    col_count = lax.axis_size("col")
    devices = row_count * col_count
    share, unknowns = normal_matrix.shape
    rows = unknowns // row_count
    steps = 4

    tile, lane = new_index // TILE, new_index % TILE
    within_col = tile // col_count * TILE + lane
    column_places = (within_col // share * col_count + tile % col_count) * share + within_col % share
    within_row = tile // row_count * TILE + lane
    owner, m = within_row // share, within_row % share
    spot = jnp.zeros_like(m)
    start = 0
    for span in SPANS:
        spot = jnp.where((m >= start) & (m < start + span), start * col_count + owner * span + m - start, spot)
        start += span
    row_places = tile % row_count * rows + spot
    column_places = column_places.reshape(steps, 1, unknowns // steps)
    row_places = row_places.reshape(steps, 1, unknowns // steps)

    along = lambda x: lax.all_to_all(x, "row", split_axis=0, concat_axis=0, tiled=True)
    flip = lambda x, bits: lax.ppermute(x, "col", [(i, i ^ bits) for i in range(col_count)])
    groups = [list(range(p, col_count, 2)) for p in range(2)]
    widths = [s * col_count for s in SPANS]

    outgoing = group_columns(normal_matrix, column_places, devices)
    arrived = lax.all_to_all(outgoing, ("row", "col"), split_axis=0, concat_axis=0, tiled=True)
    v_hi = lax.reduce_precision(check_vectors, 8, 7)
    v_lo = (check_vectors - v_hi).astype(jnp.bfloat16)
    v_hi = v_hi.astype(jnp.bfloat16)
    me = lax.axis_index("col").astype(jnp.int32)

    chosen = group_rows(arrived, row_places, row_count, share, widths)

    tile_layout = None
    sums = []
    last = arrived
    offset = 0
    for q, span in enumerate(SPANS):
        final = q == len(SPANS) - 1
        send, _ = lax.optimization_barrier((chosen[q], last))
        last = along(send)
        piece = last
        if sums:
            piece, sums[-1] = lax.optimization_barrier((last, sums[-1]))
        where = jnp.stack([me % 2, jnp.zeros_like(me) if final else me // 2])
        tile_layout, other, mine = tile_and_product(piece, v_hi, v_lo, where, tile_layout, col_count, share, offset)
        offset += span
        both = mine + flip(other, 1)
        if final:
            parts = lax.all_to_all(both, "col", split_axis=0, concat_axis=0, axis_index_groups=groups, tiled=True)
            sums.append(parts.sum(axis=0))
        else:
            near = both[0:2]
            for y in range(1, col_count // 4):
                near = near + flip(both[2 * y:2 * y + 2], 4 * y)
            sums.append(near[0] + flip(near[1], 2))
    return tile_layout.reshape(rows, unknowns // col_count), jnp.concatenate(sums, axis=0)


def solution(mesh):
    return jax.shard_map(
        shards,
        mesh=mesh,
        in_specs=(P(("row", "col"), None), P(), P("col", None)),
        out_specs=(P("row", "col"), P(("row", "col"), None)),
        check_vma=False,
    )
```

```python
import jax
import jax.numpy as jnp
from jax import lax
from jax.experimental import pallas as pl
from jax.experimental.pallas import tpu as pltpu
from jax.sharding import PartitionSpec as P


TILE = 128
LANES = 128
SUB = 8
VMEM = 56 * 1024 * 1024
SPANS = (48, 40, 24)
STEPS = 8


def params():
    return pltpu.CompilerParams(vmem_limit_bytes=VMEM)


def group_columns(slab, places, devices):
    share, unknowns = slab.shape
    steps, _, width = places.shape
    keep = share - SUB
    chunk = LANES - share
    outs = 4
    per = devices // outs

    def kernel(pos_ref, x_ref, out_ref, turned, spread):
        step = pl.program_id(0)

        @pl.when(step < steps)
        def _():
            for b in range(width // LANES):
                turned[b * LANES:(b + 1) * LANES, :share] = x_ref[:, b * LANES:(b + 1) * LANES].T

            for u in range(width):
                spread[pl.ds(pos_ref[0, 0, u], 1), :] = turned[u:u + 1, :]

        @pl.when(step >= steps)
        def _():
            first = (step - steps) * per

            def pack(i, carry):
                for u in range(8):
                    b = i * 8 + u
                    x = spread[pl.ds(pl.multiple_of((first + b) * share, SUB), share), :].T
                    out_ref[b, :, :share] = x[:keep]
                    for k in range(share // chunk):
                        out_ref[b, SUB * k:SUB * k + SUB, share:] = x[keep:share, chunk * k:chunk * (k + 1)]
                return carry

            lax.fori_loop(0, per // 8, pack, 0)

    return pl.pallas_call(
        kernel,
        grid=(steps + outs,),
        in_specs=[
            pl.BlockSpec((1, 1, width), lambda g: (jnp.minimum(g, steps - 1), 0, 0), memory_space=pltpu.SMEM),
            pl.BlockSpec((share, width), lambda g: (0, jnp.minimum(g, steps - 1))),
        ],
        out_specs=pl.BlockSpec((per, keep, LANES), lambda g: (jnp.maximum(g - steps, 0), 0, 0)),
        scratch_shapes=[
            pltpu.VMEM((width, LANES), jnp.float32),
            pltpu.VMEM((unknowns, LANES), jnp.float32),
        ],
        out_shape=jax.ShapeDtypeStruct((devices, keep, LANES), jnp.float32),
        compiler_params=params(),
        name="group_columns",
    )(places, slab)


def group_rows(blocks, places, groups, share, widths):
    devices, keep, _ = blocks.shape
    unknowns = devices * share
    chunk = LANES - share
    steps = places.shape[0]
    per = devices // steps
    rows = unknowns // groups
    starts = [sum(widths[:i]) for i in range(len(widths))]
    outs = 4
    each = groups // outs

    def kernel(pos_ref, x_ref, *refs):
        out_refs, (extra, spread) = refs[:-2], refs[-2:]
        step = pl.program_id(0)

        @pl.when(step < steps)
        def _():
            def unpack(i, carry):
                for u in range(8):
                    b = i * 8 + u
                    at = pl.multiple_of(b * SUB, SUB)
                    for k in range(share // chunk):
                        extra[pl.ds(at, SUB), chunk * k:chunk * (k + 1)] = x_ref[b, SUB * k:SUB * k + SUB, share:]
                return carry

            lax.fori_loop(0, per // 8, unpack, 0)

            for b in range(per):
                start = b * share
                for u in range(keep):
                    spread[pl.ds(pos_ref[0, 0, start + u], 1), :] = x_ref[b, u:u + 1, :]
                for u in range(SUB):
                    at = b * SUB + u
                    spread[pl.ds(pos_ref[0, 0, start + keep + u], 1), :] = extra[at:at + 1, :]

        @pl.when(step >= steps)
        def _():
            def turn(e, carry):
                g = (step - steps) * each + e
                for ref, start, width in zip(out_refs, starts, widths):
                    for k in range(width // LANES):
                        at = pl.multiple_of(g * rows + start + k * LANES, LANES)
                        ref[e, :, k * LANES:(k + 1) * LANES] = spread[pl.ds(at, LANES), :].T[:share]
                return carry

            lax.fori_loop(0, each, turn, 0)

    late = lambda g: (jnp.maximum(g - steps, 0), 0, 0)
    early = lambda g: (jnp.minimum(g, steps - 1), 0, 0)
    return pl.pallas_call(
        kernel,
        grid=(steps + outs,),
        in_specs=[
            pl.BlockSpec((1, 1, per * share), early, memory_space=pltpu.SMEM),
            pl.BlockSpec((per, keep, LANES), early),
        ],
        out_specs=[pl.BlockSpec((each, share, w), late) for w in widths],
        scratch_shapes=[
            pltpu.VMEM((per * SUB, LANES), jnp.float32),
            pltpu.VMEM((unknowns, LANES), jnp.float32),
        ],
        out_shape=[jax.ShapeDtypeStruct((groups, share, w), jnp.float32) for w in widths],
        compiler_params=params(),
        name="group_rows",
    )(places, blocks)


def tile_and_product(turned, v_hi, v_lo, where, tile, cols, share, offset):
    groups, _, rows = turned.shape
    span = rows // cols
    columns, width = v_hi.shape
    steps = 4
    wide = width // steps
    pairs = cols // 2

    def kernel(where_ref, x_ref, hi_ref, lo_ref, *refs):
        tile_ref, other_ref, mine_ref, x_hi, x_lo, held, sem = refs[-7:]
        step = pl.program_id(0)
        store = pltpu.make_async_copy(held, tile_ref.at[:, offset:offset + span, :], sem)

        @pl.when(step == 0)
        def _():
            for k in range(rows // LANES):
                x = x_ref[:, :, k * LANES:(k + 1) * LANES].reshape(columns, LANES).T
                hi = x.astype(jnp.bfloat16)
                x_hi[k * LANES:(k + 1) * LANES, :] = hi
                x_lo[k * LANES:(k + 1) * LANES, :] = (x - hi.astype(jnp.float32)).astype(jnp.bfloat16)
                for s in range(0, LANES, SUB):
                    c, m = divmod(k * LANES + s, span)
                    held[c, m:m + SUB, :] = x[s:s + SUB]
            store.start()

        part = (
            jnp.dot(x_hi[...], hi_ref[...], preferred_element_type=jnp.float32)
            + jnp.dot(x_hi[...], lo_ref[...], preferred_element_type=jnp.float32)
            + jnp.dot(x_lo[...], hi_ref[...], preferred_element_type=jnp.float32)
        )
        even = where_ref[0] == 0
        for c in range(pairs):
            slot = c ^ where_ref[1]
            first = part[2 * c * span:(2 * c + 1) * span]
            second = part[(2 * c + 1) * span:(2 * c + 2) * span]
            other_ref[slot] = jnp.where(even, second, first)
            mine_ref[slot] = jnp.where(even, first, second)

        @pl.when(step == steps - 1)
        def _():
            store.wait()

    half = jax.ShapeDtypeStruct((pairs, span, width), jnp.float32)
    half_spec = pl.BlockSpec((pairs, span, wide), lambda g, where: (0, 0, g))
    in_specs = [pl.BlockSpec((groups, share, rows), lambda g, where: (0, 0, 0))]
    in_specs += [pl.BlockSpec((columns, wide), lambda g, where: (0, g))] * 2
    operands = [where, turned, v_hi, v_lo]
    aliases = {}
    if tile is not None:
        aliases = {len(operands): 0}
        operands.append(tile)
        in_specs.append(pl.BlockSpec(memory_space=pl.ANY))
    return pl.pallas_call(
        kernel,
        grid_spec=pltpu.PrefetchScalarGridSpec(
            num_scalar_prefetch=1,
            grid=(steps,),
            in_specs=in_specs,
            out_specs=[pl.BlockSpec(memory_space=pl.ANY), half_spec, half_spec],
            scratch_shapes=[
                pltpu.VMEM((rows, columns), jnp.bfloat16),
                pltpu.VMEM((rows, columns), jnp.bfloat16),
                pltpu.VMEM((cols, span, columns), jnp.float32),
                pltpu.SemaphoreType.DMA,
            ],
        ),
        out_shape=[jax.ShapeDtypeStruct((cols, share, columns), jnp.float32), half, half],
        input_output_aliases=aliases,
        compiler_params=params(),
        cost_estimate=pl.CostEstimate(flops=6 * rows * columns * width, bytes_accessed=8 * rows * columns, transcendentals=0),
    )(*operands)


def shards(normal_matrix, new_index, check_vectors):
    row_count = lax.axis_size("row")
    col_count = lax.axis_size("col")
    devices = row_count * col_count
    share, unknowns = normal_matrix.shape
    rows = unknowns // row_count
    steps = STEPS

    tile, lane = new_index // TILE, new_index % TILE
    within_col = tile // col_count * TILE + lane
    column_places = (within_col // share * col_count + tile % col_count) * share + within_col % share
    within_row = tile // row_count * TILE + lane
    owner, m = within_row // share, within_row % share
    spot = jnp.zeros_like(m)
    start = 0
    for span in SPANS:
        spot = jnp.where((m >= start) & (m < start + span), start * col_count + owner * span + m - start, spot)
        start += span
    row_places = tile % row_count * rows + spot
    column_places = column_places.reshape(steps, 1, unknowns // steps)
    row_places = row_places.reshape(steps, 1, unknowns // steps)

    along = lambda x: lax.all_to_all(x, "row", split_axis=0, concat_axis=0, tiled=True)
    flip = lambda x, bits: lax.ppermute(x, "col", [(i, i ^ bits) for i in range(col_count)])
    groups = [list(range(p, col_count, 2)) for p in range(2)]
    widths = [s * col_count for s in SPANS]

    outgoing = group_columns(normal_matrix, column_places, devices)
    arrived = lax.all_to_all(outgoing, ("row", "col"), split_axis=0, concat_axis=0, tiled=True)
    v_hi = lax.reduce_precision(check_vectors, 8, 7)
    v_lo = (check_vectors - v_hi).astype(jnp.bfloat16)
    v_hi = v_hi.astype(jnp.bfloat16)
    me = lax.axis_index("col").astype(jnp.int32)

    chosen = group_rows(arrived, row_places, row_count, share, widths)

    tile_layout = None
    sums = []
    last, held = arrived, None
    offset = 0
    for q, span in enumerate(SPANS):
        final = q == len(SPANS) - 1
        send, _ = lax.optimization_barrier((chosen[q], last))
        last = along(send)
        piece = last
        if held is not None:
            piece, _ = lax.optimization_barrier((last, held))
        where = jnp.stack([me % 2, jnp.zeros_like(me) if final else me // 2])
        tile_layout, other, mine = tile_and_product(piece, v_hi, v_lo, where, tile_layout, col_count, share, offset)
        offset += span
        both = mine + flip(other, 1)
        if final:
            parts = lax.all_to_all(both, "col", split_axis=0, concat_axis=0, axis_index_groups=groups, tiled=True)
            sums.append(parts.sum(axis=0))
        else:
            near = both[0:2]
            for y in range(1, col_count // 4):
                got = flip(both[2 * y:2 * y + 2], 4 * y)
                near = near + got
            held = both if q == len(SPANS) - 2 else near
            got = flip(near[1], 2)
            sums.append(near[0] + got)
    return tile_layout.reshape(rows, unknowns // col_count), jnp.concatenate(sums, axis=0)


def solution(mesh):
    return jax.shard_map(
        shards,
        mesh=mesh,
        in_specs=(P(("row", "col"), None), P(), P("col", None)),
        out_specs=(P("row", "col"), P(("row", "col"), None)),
        check_vma=False,
    )
```

```python
import jax
import jax.numpy as jnp
from jax import lax
from jax.experimental import pallas as pl
from jax.experimental.pallas import tpu as pltpu
from jax.sharding import PartitionSpec as P


TILE = 128
LANES = 128
SUB = 8
VMEM = 24 * 1024 * 1024
SPANS = (48, 40, 24)
STEPS = 8


def params():
    return pltpu.CompilerParams(vmem_limit_bytes=VMEM)


def group_columns(slab, places, devices):
    share, unknowns = slab.shape
    steps, _, width = places.shape
    keep = share - SUB
    chunk = LANES - share
    outs = 4
    per = devices // outs

    def kernel(pos_ref, x_ref, out_ref, turned, spread):
        step = pl.program_id(0)

        @pl.when(step < steps)
        def _():
            for b in range(width // LANES):
                turned[b * LANES:(b + 1) * LANES, :share] = x_ref[:, b * LANES:(b + 1) * LANES].T

            for u in range(width):
                spread[pl.ds(pos_ref[0, 0, u], 1), :] = turned[u:u + 1, :]

        @pl.when(step >= steps)
        def _():
            first = (step - steps) * per

            def pack(i, carry):
                for u in range(8):
                    b = i * 8 + u
                    x = spread[pl.ds(pl.multiple_of((first + b) * share, SUB), share), :].T
                    out_ref[b, :, :share] = x[:keep]
                    for k in range(share // chunk):
                        out_ref[b, SUB * k:SUB * k + SUB, share:] = x[keep:share, chunk * k:chunk * (k + 1)]
                return carry

            lax.fori_loop(0, per // 8, pack, 0)

    return pl.pallas_call(
        kernel,
        grid=(steps + outs,),
        in_specs=[
            pl.BlockSpec((1, 1, width), lambda g: (jnp.minimum(g, steps - 1), 0, 0), memory_space=pltpu.SMEM),
            pl.BlockSpec((share, width), lambda g: (0, jnp.minimum(g, steps - 1))),
        ],
        out_specs=pl.BlockSpec((per, keep, LANES), lambda g: (jnp.maximum(g - steps, 0), 0, 0)),
        scratch_shapes=[
            pltpu.VMEM((width, LANES), jnp.float32),
            pltpu.VMEM((unknowns, LANES), jnp.float32),
        ],
        out_shape=jax.ShapeDtypeStruct((devices, keep, LANES), jnp.float32),
        compiler_params=params(),
        name="group_columns",
    )(places, slab)


def group_rows(blocks, places, groups, share, widths):
    devices, keep, _ = blocks.shape
    unknowns = devices * share
    chunk = LANES - share
    steps = places.shape[0]
    per = devices // steps
    rows = unknowns // groups
    starts = [sum(widths[:i]) for i in range(len(widths))]
    outs = 4
    each = groups // outs

    def kernel(pos_ref, x_ref, *refs):
        out_refs, (extra, spread) = refs[:-2], refs[-2:]
        step = pl.program_id(0)

        @pl.when(step < steps)
        def _():
            for b in range(per):
                start = b * share
                for k in range(share // chunk):
                    extra[b * SUB:(b + 1) * SUB, chunk * k:chunk * (k + 1)] = x_ref[b, SUB * k:SUB * k + SUB, share:]
                for u in range(keep):
                    spread[pl.ds(pos_ref[0, 0, start + u], 1), :] = x_ref[b, u:u + 1, :]
                for u in range(SUB):
                    at = b * SUB + u
                    spread[pl.ds(pos_ref[0, 0, start + keep + u], 1), :] = extra[at:at + 1, :]

        @pl.when(step >= steps)
        def _():
            def turn(e, carry):
                g = (step - steps) * each + e
                for ref, start, width in zip(out_refs, starts, widths):
                    for k in range(width // LANES):
                        at = pl.multiple_of(g * rows + start + k * LANES, LANES)
                        ref[e, :, k * LANES:(k + 1) * LANES] = spread[pl.ds(at, LANES), :].T[:share]
                return carry

            lax.fori_loop(0, each, turn, 0)

    late = lambda g: (jnp.maximum(g - steps, 0), 0, 0)
    early = lambda g: (jnp.minimum(g, steps - 1), 0, 0)
    return pl.pallas_call(
        kernel,
        grid=(steps + outs,),
        in_specs=[
            pl.BlockSpec((1, 1, per * share), early, memory_space=pltpu.SMEM),
            pl.BlockSpec((per, keep, LANES), early),
        ],
        out_specs=[pl.BlockSpec((each, share, w), late) for w in widths],
        scratch_shapes=[
            pltpu.VMEM((per * SUB, LANES), jnp.float32),
            pltpu.VMEM((unknowns, LANES), jnp.float32),
        ],
        out_shape=[jax.ShapeDtypeStruct((groups, share, w), jnp.float32) for w in widths],
        compiler_params=params(),
        name="group_rows",
    )(places, blocks)


def tile_and_product(turned, v_hi, v_lo, where, tile, cols, share, offset):
    groups, _, rows = turned.shape
    span = rows // cols
    columns, width = v_hi.shape
    steps = 4
    wide = width // steps
    pairs = cols // 2

    def kernel(where_ref, x_ref, hi_ref, lo_ref, *refs):
        tile_ref, other_ref, mine_ref, x_in, x_hi, x_lo, held, x_sem, sem = refs[-9:]
        step = pl.program_id(0)
        store = pltpu.make_async_copy(held, tile_ref.at[:, offset:offset + span, :], sem)

        @pl.when(step == 0)
        def _():
            fetch = pltpu.make_async_copy(x_ref, x_in, x_sem)
            fetch.start()
            fetch.wait()
            for k in range(rows // LANES):
                x = x_in[:, :, k * LANES:(k + 1) * LANES].reshape(columns, LANES).T
                hi = x.astype(jnp.bfloat16)
                x_hi[k * LANES:(k + 1) * LANES, :] = hi
                x_lo[k * LANES:(k + 1) * LANES, :] = (x - hi.astype(jnp.float32)).astype(jnp.bfloat16)
                for s in range(0, LANES, SUB):
                    c, m = divmod(k * LANES + s, span)
                    held[c, m:m + SUB, :] = x[s:s + SUB]
            store.start()

        part = (
            jnp.dot(x_hi[...], hi_ref[...], preferred_element_type=jnp.float32)
            + jnp.dot(x_hi[...], lo_ref[...], preferred_element_type=jnp.float32)
            + jnp.dot(x_lo[...], hi_ref[...], preferred_element_type=jnp.float32)
        )
        even = where_ref[0] == 0
        for c in range(pairs):
            slot = c ^ where_ref[1]
            first = part[2 * c * span:(2 * c + 1) * span]
            second = part[(2 * c + 1) * span:(2 * c + 2) * span]
            other_ref[slot] = jnp.where(even, second, first)
            mine_ref[slot] = jnp.where(even, first, second)

        @pl.when(step == steps - 1)
        def _():
            store.wait()

    half = jax.ShapeDtypeStruct((pairs, span, width), jnp.float32)
    half_spec = pl.BlockSpec((pairs, span, wide), lambda g, where: (0, 0, g))
    in_specs = [pl.BlockSpec(memory_space=pl.ANY)]
    in_specs += [pl.BlockSpec((columns, wide), lambda g, where: (0, g))] * 2
    operands = [where, turned, v_hi, v_lo]
    aliases = {}
    if tile is not None:
        aliases = {len(operands): 0}
        operands.append(tile)
        in_specs.append(pl.BlockSpec(memory_space=pl.ANY))
    return pl.pallas_call(
        kernel,
        grid_spec=pltpu.PrefetchScalarGridSpec(
            num_scalar_prefetch=1,
            grid=(steps,),
            in_specs=in_specs,
            out_specs=[pl.BlockSpec(memory_space=pl.ANY), half_spec, half_spec],
            scratch_shapes=[
                pltpu.VMEM((groups, share, rows), jnp.float32),
                pltpu.VMEM((rows, columns), jnp.bfloat16),
                pltpu.VMEM((rows, columns), jnp.bfloat16),
                pltpu.VMEM((cols, span, columns), jnp.float32),
                pltpu.SemaphoreType.DMA,
                pltpu.SemaphoreType.DMA,
            ],
        ),
        out_shape=[jax.ShapeDtypeStruct((cols, share, columns), jnp.float32), half, half],
        input_output_aliases=aliases,
        compiler_params=params(),
        cost_estimate=pl.CostEstimate(flops=6 * rows * columns * width, bytes_accessed=8 * rows * columns, transcendentals=0),
    )(*operands)


def shards(normal_matrix, new_index, check_vectors):
    row_count = lax.axis_size("row")
    col_count = lax.axis_size("col")
    devices = row_count * col_count
    share, unknowns = normal_matrix.shape
    rows = unknowns // row_count
    steps = STEPS

    tile, lane = new_index // TILE, new_index % TILE
    within_col = tile // col_count * TILE + lane
    column_places = (within_col // share * col_count + tile % col_count) * share + within_col % share
    within_row = tile // row_count * TILE + lane
    owner, m = within_row // share, within_row % share
    spot = jnp.zeros_like(m)
    start = 0
    for span in SPANS:
        spot = jnp.where((m >= start) & (m < start + span), start * col_count + owner * span + m - start, spot)
        start += span
    row_places = tile % row_count * rows + spot
    column_places = column_places.reshape(steps, 1, unknowns // steps)
    row_places = row_places.reshape(steps, 1, unknowns // steps)

    along = lambda x: lax.all_to_all(x, "row", split_axis=0, concat_axis=0, tiled=True)
    flip = lambda x, bits: lax.ppermute(x, "col", [(i, i ^ bits) for i in range(col_count)])
    groups = [list(range(p, col_count, 2)) for p in range(2)]
    widths = [s * col_count for s in SPANS]

    outgoing = group_columns(normal_matrix, column_places, devices)
    arrived = lax.all_to_all(outgoing, ("row", "col"), split_axis=0, concat_axis=0, tiled=True)
    v_hi = lax.reduce_precision(check_vectors, 8, 7)
    v_lo = (check_vectors - v_hi).astype(jnp.bfloat16)
    v_hi = v_hi.astype(jnp.bfloat16)
    me = lax.axis_index("col").astype(jnp.int32)

    chosen = group_rows(arrived, row_places, row_count, share, widths)

    tile_layout = None
    sums = []
    last, held = arrived, None
    offset = 0
    for q, span in enumerate(SPANS):
        final = q == len(SPANS) - 1
        send, _ = lax.optimization_barrier((chosen[q], last))
        last = along(send)
        piece = last
        if held is not None:
            piece, _ = lax.optimization_barrier((last, held))
        turn = me // 2 if not final else me * 0
        where = jnp.stack([me % 2, turn, me * 0 + q])
        tile_layout, other, mine = tile_and_product(piece, v_hi, v_lo, where, tile_layout, col_count, share, offset)
        offset += span
        theirs = flip(other, 1)
        if final:
            both = mine + theirs
            parts = lax.all_to_all(both, "col", split_axis=0, concat_axis=0, axis_index_groups=groups, tiled=True)
            sums.append(parts.sum(axis=0))
        else:
            both = [mine[i:i + 2] + theirs[i:i + 2] for i in range(0, col_count // 2, 2)]
            near = both[0]
            for y in range(1, col_count // 4):
                got = flip(both[y], 4 * y)
                near = near + got
            held = tuple(both[1:])
            got = flip(near[1], 2)
            sums.append(near[0] + got)
    return tile_layout.reshape(rows, unknowns // col_count), jnp.concatenate(sums, axis=0)


def solution(mesh):
    return jax.shard_map(
        shards,
        mesh=mesh,
        in_specs=(P(("row", "col"), None), P(), P("col", None)),
        out_specs=(P("row", "col"), P(("row", "col"), None)),
        check_vma=False,
    )
```

```python
import jax
import jax.numpy as jnp
from jax import lax
from jax.experimental import pallas as pl
from jax.experimental.pallas import tpu as pltpu
from jax.sharding import PartitionSpec as P


TILE = 128
LANES = 128
SUB = 8
VMEM = 24 * 1024 * 1024
SPANS = (48, 40, 24)
STEPS = 8


def params():
    return pltpu.CompilerParams(vmem_limit_bytes=VMEM)


def group_columns(slab, places, devices):
    share, unknowns = slab.shape
    steps, _, width = places.shape
    keep = share - SUB
    chunk = LANES - share
    outs = 4
    per = devices // outs

    def kernel(pos_ref, x_ref, out_ref, turned, spread):
        step = pl.program_id(0)

        @pl.when(step < steps)
        def _():
            for b in range(width // LANES):
                turned[b * LANES:(b + 1) * LANES, :share] = x_ref[:, b * LANES:(b + 1) * LANES].T

            for u in range(width):
                spread[pl.ds(pos_ref[0, 0, u], 1), :] = turned[u:u + 1, :]

        @pl.when(step >= steps)
        def _():
            first = (step - steps) * per

            def pack(i, carry):
                for u in range(8):
                    b = i * 8 + u
                    x = spread[pl.ds(pl.multiple_of((first + b) * share, SUB), share), :].T
                    out_ref[b, :, :share] = x[:keep]
                    for k in range(share // chunk):
                        out_ref[b, SUB * k:SUB * k + SUB, share:] = x[keep:share, chunk * k:chunk * (k + 1)]
                return carry

            lax.fori_loop(0, per // 8, pack, 0)

    return pl.pallas_call(
        kernel,
        grid=(steps + outs,),
        in_specs=[
            pl.BlockSpec((1, 1, width), lambda g: (jnp.minimum(g, steps - 1), 0, 0), memory_space=pltpu.SMEM),
            pl.BlockSpec((share, width), lambda g: (0, jnp.minimum(g, steps - 1))),
        ],
        out_specs=pl.BlockSpec((per, keep, LANES), lambda g: (jnp.maximum(g - steps, 0), 0, 0)),
        scratch_shapes=[
            pltpu.VMEM((width, LANES), jnp.float32),
            pltpu.VMEM((unknowns, LANES), jnp.float32),
        ],
        out_shape=jax.ShapeDtypeStruct((devices, keep, LANES), jnp.float32),
        compiler_params=params(),
        name="group_columns",
    )(places, slab)


def group_rows(blocks, places, groups, share, widths):
    devices, keep, _ = blocks.shape
    unknowns = devices * share
    chunk = LANES - share
    steps = places.shape[0]
    per = devices // steps
    rows = unknowns // groups
    starts = [sum(widths[:i]) for i in range(len(widths))]
    outs = 4
    each = groups // outs

    def kernel(pos_ref, x_ref, *refs):
        out_refs, (extra, spread) = refs[:-2], refs[-2:]
        step = pl.program_id(0)

        @pl.when(step < steps)
        def _():
            for b in range(per):
                start = b * share
                for k in range(share // chunk):
                    extra[b * SUB:(b + 1) * SUB, chunk * k:chunk * (k + 1)] = x_ref[b, SUB * k:SUB * k + SUB, share:]
                for u in range(keep):
                    spread[pl.ds(pos_ref[0, 0, start + u], 1), :] = x_ref[b, u:u + 1, :]
                for u in range(SUB):
                    at = b * SUB + u
                    spread[pl.ds(pos_ref[0, 0, start + keep + u], 1), :] = extra[at:at + 1, :]

        @pl.when(step >= steps)
        def _():
            def turn(e, carry):
                g = (step - steps) * each + e
                for ref, start, width in zip(out_refs, starts, widths):
                    for k in range(width // LANES):
                        at = pl.multiple_of(g * rows + start + k * LANES, LANES)
                        ref[e, :, k * LANES:(k + 1) * LANES] = spread[pl.ds(at, LANES), :].T[:share]
                return carry

            lax.fori_loop(0, each, turn, 0)

    late = lambda g: (jnp.maximum(g - steps, 0), 0, 0)
    early = lambda g: (jnp.minimum(g, steps - 1), 0, 0)
    return pl.pallas_call(
        kernel,
        grid=(steps + outs,),
        in_specs=[
            pl.BlockSpec((1, 1, per * share), early, memory_space=pltpu.SMEM),
            pl.BlockSpec((per, keep, LANES), early),
        ],
        out_specs=[pl.BlockSpec((each, share, w), late) for w in widths],
        scratch_shapes=[
            pltpu.VMEM((per * SUB, LANES), jnp.float32),
            pltpu.VMEM((unknowns, LANES), jnp.float32),
        ],
        out_shape=[(pltpu.HBM if i else jax.ShapeDtypeStruct)((groups, share, w), jnp.float32) for i, w in enumerate(widths)],
        compiler_params=params(),
        name="group_rows",
    )(places, blocks)


def tile_and_product(turned, v_hi, v_lo, where, tile, cols, share, offset):
    groups, _, rows = turned.shape
    span = rows // cols
    columns, width = v_hi.shape
    steps = 4
    wide = width // steps
    pairs = cols // 2

    def kernel(where_ref, x_ref, hi_ref, lo_ref, *refs):
        tile_ref, other_ref, mine_ref, x_in, x_hi, x_lo, held, x_sem, sem = refs[-9:]
        step = pl.program_id(0)
        store = pltpu.make_async_copy(held, tile_ref.at[:, offset:offset + span, :], sem)

        @pl.when(step == 0)
        def _():
            fetch = pltpu.make_async_copy(x_ref, x_in, x_sem)
            fetch.start()
            fetch.wait()
            for k in range(rows // LANES):
                x = x_in[:, :, k * LANES:(k + 1) * LANES].reshape(columns, LANES).T
                hi = x.astype(jnp.bfloat16)
                x_hi[k * LANES:(k + 1) * LANES, :] = hi
                x_lo[k * LANES:(k + 1) * LANES, :] = (x - hi.astype(jnp.float32)).astype(jnp.bfloat16)
                for s in range(0, LANES, SUB):
                    c, m = divmod(k * LANES + s, span)
                    held[c, m:m + SUB, :] = x[s:s + SUB]
            store.start()

        part = (
            jnp.dot(x_hi[...], hi_ref[...], preferred_element_type=jnp.float32)
            + jnp.dot(x_hi[...], lo_ref[...], preferred_element_type=jnp.float32)
            + jnp.dot(x_lo[...], hi_ref[...], preferred_element_type=jnp.float32)
        )
        even = where_ref[0] == 0
        for c in range(pairs):
            slot = c ^ where_ref[1]
            first = part[2 * c * span:(2 * c + 1) * span]
            second = part[(2 * c + 1) * span:(2 * c + 2) * span]
            other_ref[slot] = jnp.where(even, second, first)
            mine_ref[slot] = jnp.where(even, first, second)

        @pl.when(step == steps - 1)
        def _():
            store.wait()

    half = jax.ShapeDtypeStruct((pairs, span, width), jnp.float32)
    half_spec = pl.BlockSpec((pairs, span, wide), lambda g, where: (0, 0, g))
    in_specs = [pl.BlockSpec(memory_space=pl.ANY)]
    in_specs += [pl.BlockSpec((columns, wide), lambda g, where: (0, g))] * 2
    operands = [where, turned, v_hi, v_lo]
    aliases = {}
    if tile is not None:
        aliases = {len(operands): 0}
        operands.append(tile)
        in_specs.append(pl.BlockSpec(memory_space=pl.ANY))
    return pl.pallas_call(
        kernel,
        grid_spec=pltpu.PrefetchScalarGridSpec(
            num_scalar_prefetch=1,
            grid=(steps,),
            in_specs=in_specs,
            out_specs=[pl.BlockSpec(memory_space=pl.ANY), half_spec, half_spec],
            scratch_shapes=[
                pltpu.VMEM((groups, share, rows), jnp.float32),
                pltpu.VMEM((rows, columns), jnp.bfloat16),
                pltpu.VMEM((rows, columns), jnp.bfloat16),
                pltpu.VMEM((cols, span, columns), jnp.float32),
                pltpu.SemaphoreType.DMA,
                pltpu.SemaphoreType.DMA,
            ],
        ),
        out_shape=[jax.ShapeDtypeStruct((cols, share, columns), jnp.float32), half, half],
        input_output_aliases=aliases,
        compiler_params=params(),
        cost_estimate=pl.CostEstimate(flops=6 * rows * columns * width, bytes_accessed=8 * rows * columns, transcendentals=0),
    )(*operands)


def shards(normal_matrix, new_index, check_vectors):
    row_count = lax.axis_size("row")
    col_count = lax.axis_size("col")
    devices = row_count * col_count
    share, unknowns = normal_matrix.shape
    rows = unknowns // row_count
    steps = STEPS

    tile, lane = new_index // TILE, new_index % TILE
    within_col = tile // col_count * TILE + lane
    column_places = (within_col // share * col_count + tile % col_count) * share + within_col % share
    within_row = tile // row_count * TILE + lane
    owner, m = within_row // share, within_row % share
    spot = jnp.zeros_like(m)
    start = 0
    for span in SPANS:
        spot = jnp.where((m >= start) & (m < start + span), start * col_count + owner * span + m - start, spot)
        start += span
    row_places = tile % row_count * rows + spot
    column_places = column_places.reshape(steps, 1, unknowns // steps)
    row_places = row_places.reshape(steps, 1, unknowns // steps)

    along = lambda x: lax.all_to_all(x, "row", split_axis=0, concat_axis=0, tiled=True)
    flip = lambda x, bits: lax.ppermute(x, "col", [(i, i ^ bits) for i in range(col_count)])
    groups = [list(range(p, col_count, 2)) for p in range(2)]
    widths = [s * col_count for s in SPANS]

    in_hbm = lambda x: pltpu.with_memory_space_constraint(x, pltpu.HBM)
    outgoing = group_columns(in_hbm(normal_matrix), column_places, devices)
    arrived = lax.all_to_all(outgoing, ("row", "col"), split_axis=0, concat_axis=0, tiled=True)
    v_hi = lax.reduce_precision(check_vectors, 8, 7)
    v_lo = (check_vectors - v_hi).astype(jnp.bfloat16)
    v_hi = v_hi.astype(jnp.bfloat16)
    me = lax.axis_index("col").astype(jnp.int32)

    chosen = group_rows(arrived, row_places, row_count, share, widths)

    tile_layout = None
    sums = []
    last, held = arrived, None
    offset = 0
    for q, span in enumerate(SPANS):
        final = q == len(SPANS) - 1
        send, _ = lax.optimization_barrier((chosen[q], last))
        last = along(send)
        piece = last
        if held is not None:
            piece, _ = lax.optimization_barrier((last, held))
        turn = me // 2 if not final else me * 0
        where = jnp.stack([me % 2, turn, me * 0 + q])
        tile_layout, other, mine = tile_and_product(
            piece, in_hbm(v_hi), in_hbm(v_lo), where, tile_layout, col_count, share, offset
        )
        offset += span
        theirs = flip(other, 1)
        if final:
            both = mine + theirs
            parts = lax.all_to_all(both, "col", split_axis=0, concat_axis=0, axis_index_groups=groups, tiled=True)
            sums.append(parts.sum(axis=0))
        else:
            both = [mine[i:i + 2] + theirs[i:i + 2] for i in range(0, col_count // 2, 2)]
            near = both[0]
            for y in range(1, col_count // 4):
                got = flip(both[y], 4 * y)
                near = near + got
            held = tuple(both[1:])
            got = flip(near[1], 2)
            sums.append(near[0] + got)
    return tile_layout.reshape(rows, unknowns // col_count), jnp.concatenate(sums, axis=0)


def solution(mesh):
    return jax.shard_map(
        shards,
        mesh=mesh,
        in_specs=(P(("row", "col"), None), P(), P("col", None)),
        out_specs=(P("row", "col"), P(("row", "col"), None)),
        check_vma=False,
    )
```

```python
import jax
import jax.numpy as jnp
from jax import lax
from jax.experimental import pallas as pl
from jax.experimental.pallas import tpu as pltpu
from jax.sharding import PartitionSpec as P


TILE = 128
LANES = 128
SUB = 8
VMEM = 24 * 1024 * 1024
SPANS = (48, 40, 24)
STEPS = 8


def params():
    return pltpu.CompilerParams(vmem_limit_bytes=VMEM)


def group_columns(slab, places, devices):
    share, unknowns = slab.shape
    steps, _, width = places.shape
    keep = share - SUB
    chunk = LANES - share

    def kernel(pos_ref, x_ref, out_ref, turned, spread):
        step = pl.program_id(0)

        for b in range(width // LANES + 1):
            if b < width // LANES:
                turned[b * LANES:(b + 1) * LANES, :share] = x_ref[:, b * LANES:(b + 1) * LANES].T
            if b > 0:
                for u in range((b - 1) * LANES, b * LANES):
                    spread[pl.ds(pos_ref[0, 0, u], 1), :] = turned[u:u + 1, :]

        @pl.when(step == steps - 1)
        def _():
            def pack(i, carry):
                for u in range(16):
                    b = i * 16 + u
                    x = spread[pl.ds(pl.multiple_of(b * share, SUB), share), :].T
                    out_ref[b, :, :share] = x[:keep]
                    for k in range(share // chunk):
                        out_ref[b, SUB * k:SUB * k + SUB, share:] = x[keep:share, chunk * k:chunk * (k + 1)]
                return carry

            lax.fori_loop(0, devices // 16, pack, 0)

    return pl.pallas_call(
        kernel,
        grid=(steps,),
        in_specs=[
            pl.BlockSpec((1, 1, width), lambda g: (g, 0, 0), memory_space=pltpu.SMEM),
            pl.BlockSpec((share, width), lambda g: (0, g)),
        ],
        out_specs=pl.BlockSpec(memory_space=pltpu.VMEM),
        scratch_shapes=[
            pltpu.VMEM((width, LANES), jnp.float32),
            pltpu.VMEM((unknowns, LANES), jnp.float32),
        ],
        out_shape=pltpu.VMEM((devices, keep, LANES), jnp.float32),
        compiler_params=params(),
        name="group_columns",
    )(places, slab)


def group_rows(blocks, places, groups, share, widths):
    devices, keep, _ = blocks.shape
    unknowns = devices * share
    chunk = LANES - share
    steps = places.shape[0]
    per = devices // steps
    rows = unknowns // groups
    starts = [sum(widths[:i]) for i in range(len(widths))]
    outs = 4
    each = groups // outs

    def kernel(pos_ref, x_ref, *refs):
        out_refs, (extra, spread) = refs[:-2], refs[-2:]
        step = pl.program_id(0)

        @pl.when(step < steps)
        def _():
            for b in range(per):
                start = b * share
                for k in range(share // chunk):
                    extra[b * SUB:(b + 1) * SUB, chunk * k:chunk * (k + 1)] = x_ref[b, SUB * k:SUB * k + SUB, share:]
                for u in range(keep):
                    spread[pl.ds(pos_ref[0, 0, start + u], 1), :] = x_ref[b, u:u + 1, :]
                for u in range(SUB):
                    at = b * SUB + u
                    spread[pl.ds(pos_ref[0, 0, start + keep + u], 1), :] = extra[at:at + 1, :]

        @pl.when(step >= steps)
        def _():
            def turn(e, carry):
                g = (step - steps) * each + e
                for ref, start, width in zip(out_refs, starts, widths):
                    for k in range(width // LANES):
                        at = pl.multiple_of(g * rows + start + k * LANES, LANES)
                        ref[e, :, k * LANES:(k + 1) * LANES] = spread[pl.ds(at, LANES), :].T[:share]
                return carry

            lax.fori_loop(0, each, turn, 0)

    late = lambda g: (jnp.maximum(g - steps, 0), 0, 0)
    early = lambda g: (jnp.minimum(g, steps - 1), 0, 0)
    return pl.pallas_call(
        kernel,
        grid=(steps + outs,),
        in_specs=[
            pl.BlockSpec((1, 1, per * share), early, memory_space=pltpu.SMEM),
            pl.BlockSpec((per, keep, LANES), early),
        ],
        out_specs=[pl.BlockSpec((each, share, w), late) for w in widths],
        scratch_shapes=[
            pltpu.VMEM((per * SUB, LANES), jnp.float32),
            pltpu.VMEM((unknowns, LANES), jnp.float32),
        ],
        out_shape=[pltpu.HBM((groups, share, w), jnp.float32) for w in widths],
        compiler_params=params(),
        name="group_rows",
    )(places, blocks)


def tile_and_product(turned, v_hi, v_lo, where, tile, cols, share, offset):
    groups, _, rows = turned.shape
    span = rows // cols
    columns, width = v_hi.shape
    steps = 4
    wide = width // steps
    pairs = cols // 2

    def kernel(where_ref, x_ref, hi_ref, lo_ref, *refs):
        tile_ref, other_ref, mine_ref, x_in, x_hi, x_lo, held, x_sem, sem = refs[-9:]
        step = pl.program_id(0)
        store = pltpu.make_async_copy(held, tile_ref.at[:, offset:offset + span, :], sem)

        @pl.when(step == 0)
        def _():
            fetch = pltpu.make_async_copy(x_ref, x_in, x_sem)
            fetch.start()
            fetch.wait()
            for k in range(rows // LANES):
                x = x_in[:, :, k * LANES:(k + 1) * LANES].reshape(columns, LANES).T
                hi = x.astype(jnp.bfloat16)
                x_hi[k * LANES:(k + 1) * LANES, :] = hi
                x_lo[k * LANES:(k + 1) * LANES, :] = (x - hi.astype(jnp.float32)).astype(jnp.bfloat16)
                for s in range(0, LANES, SUB):
                    c, m = divmod(k * LANES + s, span)
                    held[c, m:m + SUB, :] = x[s:s + SUB]
            store.start()

        part = (
            jnp.dot(x_hi[...], hi_ref[...], preferred_element_type=jnp.float32)
            + jnp.dot(x_hi[...], lo_ref[...], preferred_element_type=jnp.float32)
            + jnp.dot(x_lo[...], hi_ref[...], preferred_element_type=jnp.float32)
        )
        even = where_ref[0] == 0
        for c in range(pairs):
            slot = c ^ where_ref[1]
            first = part[2 * c * span:(2 * c + 1) * span]
            second = part[(2 * c + 1) * span:(2 * c + 2) * span]
            other_ref[slot] = jnp.where(even, second, first)
            mine_ref[slot] = jnp.where(even, first, second)

        @pl.when(step == steps - 1)
        def _():
            store.wait()

    half = jax.ShapeDtypeStruct((pairs, span, width), jnp.float32)
    half_spec = pl.BlockSpec((pairs, span, wide), lambda g, where: (0, 0, g))
    in_specs = [pl.BlockSpec(memory_space=pl.ANY)]
    in_specs += [pl.BlockSpec((columns, wide), lambda g, where: (0, g))] * 2
    operands = [where, turned, v_hi, v_lo]
    aliases = {}
    if tile is not None:
        aliases = {len(operands): 0}
        operands.append(tile)
        in_specs.append(pl.BlockSpec(memory_space=pl.ANY))
    return pl.pallas_call(
        kernel,
        grid_spec=pltpu.PrefetchScalarGridSpec(
            num_scalar_prefetch=1,
            grid=(steps,),
            in_specs=in_specs,
            out_specs=[pl.BlockSpec(memory_space=pl.ANY), half_spec, half_spec],
            scratch_shapes=[
                pltpu.VMEM((groups, share, rows), jnp.float32),
                pltpu.VMEM((rows, columns), jnp.bfloat16),
                pltpu.VMEM((rows, columns), jnp.bfloat16),
                pltpu.VMEM((cols, span, columns), jnp.float32),
                pltpu.SemaphoreType.DMA,
                pltpu.SemaphoreType.DMA,
            ],
        ),
        out_shape=[jax.ShapeDtypeStruct((cols, share, columns), jnp.float32), half, half],
        input_output_aliases=aliases,
        compiler_params=params(),
        cost_estimate=pl.CostEstimate(flops=6 * rows * columns * width, bytes_accessed=8 * rows * columns, transcendentals=0),
    )(*operands)


def shards(normal_matrix, new_index, check_vectors):
    row_count = lax.axis_size("row")
    col_count = lax.axis_size("col")
    devices = row_count * col_count
    share, unknowns = normal_matrix.shape
    rows = unknowns // row_count
    steps = STEPS

    tile, lane = new_index // TILE, new_index % TILE
    within_col = tile // col_count * TILE + lane
    column_places = (within_col // share * col_count + tile % col_count) * share + within_col % share
    within_row = tile // row_count * TILE + lane
    owner, m = within_row // share, within_row % share
    spot = jnp.zeros_like(m)
    start = 0
    for span in SPANS:
        spot = jnp.where((m >= start) & (m < start + span), start * col_count + owner * span + m - start, spot)
        start += span
    row_places = tile % row_count * rows + spot
    column_places = column_places.reshape(steps, 1, unknowns // steps)
    row_places = row_places.reshape(steps, 1, unknowns // steps)

    along = lambda x: lax.all_to_all(x, "row", split_axis=0, concat_axis=0, tiled=True)
    flip = lambda x, bits: lax.ppermute(x, "col", [(i, i ^ bits) for i in range(col_count)])
    groups = [list(range(p, col_count, 2)) for p in range(2)]
    widths = [s * col_count for s in SPANS]

    in_hbm = lambda x: pltpu.with_memory_space_constraint(x, pltpu.HBM)
    outgoing = group_columns(in_hbm(normal_matrix), column_places, devices)
    arrived = lax.all_to_all(outgoing, ("row", "col"), split_axis=0, concat_axis=0, tiled=True)
    v_hi = lax.reduce_precision(check_vectors, 8, 7)
    v_lo = (check_vectors - v_hi).astype(jnp.bfloat16)
    v_hi = v_hi.astype(jnp.bfloat16)
    me = lax.axis_index("col").astype(jnp.int32)

    chosen = group_rows(arrived, row_places, row_count, share, widths)

    tile_layout = None
    sums = []
    last, held = arrived, None
    offset = 0
    for q, span in enumerate(SPANS):
        final = q == len(SPANS) - 1
        send, _ = lax.optimization_barrier((chosen[q], last))
        last = along(send)
        piece = last
        seat = me
        if held is not None:
            piece, _ = lax.optimization_barrier((last, held))
            seat, _ = lax.optimization_barrier((me, held))
        where = jnp.stack([seat % 2, jnp.zeros_like(seat) if final else seat // 2])
        tile_layout, other, mine = tile_and_product(
            piece, in_hbm(v_hi), in_hbm(v_lo), where, tile_layout, col_count, share, offset
        )
        offset += span
        theirs = flip(other, 1)
        if final:
            both = mine + theirs
            parts = lax.all_to_all(both, "col", split_axis=0, concat_axis=0, axis_index_groups=groups, tiled=True)
            sums.append(parts.sum(axis=0))
        else:
            both = [mine[i:i + 2] + theirs[i:i + 2] for i in range(0, col_count // 2, 2)]
            near = both[0]
            for y in range(1, col_count // 4):
                got = flip(both[y], 4 * y)
                near = near + got
            held = tuple(both[1:])
            got = flip(near[1], 2)
            sums.append(near[0] + got)
    return tile_layout.reshape(rows, unknowns // col_count), jnp.concatenate(sums, axis=0)


def solution(mesh):
    return jax.shard_map(
        shards,
        mesh=mesh,
        in_specs=(P(("row", "col"), None), P(), P("col", None)),
        out_specs=(P("row", "col"), P(("row", "col"), None)),
        check_vma=False,
    )
```

```python
import jax
import jax.numpy as jnp
from jax import lax
from jax.experimental import pallas as pl
from jax.experimental.pallas import tpu as pltpu
from jax.sharding import PartitionSpec as P


TILE = 128
LANES = 128
SUB = 8
VMEM = 24 * 1024 * 1024
SPANS = (48, 40, 24)
STEPS = 8


def params():
    return pltpu.CompilerParams(vmem_limit_bytes=VMEM)


def group_columns(slab, places, devices):
    share, unknowns = slab.shape
    steps, _, width = places.shape
    keep = share - SUB
    chunk = LANES - share

    def kernel(pos_ref, x_ref, out_ref, turned, spread):
        step = pl.program_id(0)

        for b in range(width // LANES + 1):
            if b < width // LANES:
                turned[b * LANES:(b + 1) * LANES, :share] = x_ref[:, b * LANES:(b + 1) * LANES].T
            if b > 0:
                for u in range((b - 1) * LANES, b * LANES):
                    spread[pl.ds(pos_ref[0, 0, u], 1), :] = turned[u:u + 1, :]

        @pl.when(step == steps - 1)
        def _():
            def pack(i, carry):
                for u in range(16):
                    b = i * 16 + u
                    x = spread[pl.ds(pl.multiple_of(b * share, SUB), share), :].T
                    out_ref[b, :, :share] = x[:keep]
                    for k in range(share // chunk):
                        out_ref[b, SUB * k:SUB * k + SUB, share:] = x[keep:share, chunk * k:chunk * (k + 1)]
                return carry

            lax.fori_loop(0, devices // 16, pack, 0)

    return pl.pallas_call(
        kernel,
        grid=(steps,),
        in_specs=[
            pl.BlockSpec((1, 1, width), lambda g: (g, 0, 0), memory_space=pltpu.SMEM),
            pl.BlockSpec((share, width), lambda g: (0, g)),
        ],
        out_specs=pl.BlockSpec(memory_space=pltpu.VMEM),
        scratch_shapes=[
            pltpu.VMEM((width, LANES), jnp.float32),
            pltpu.VMEM((unknowns, LANES), jnp.float32),
        ],
        out_shape=pltpu.VMEM((devices, keep, LANES), jnp.float32),
        compiler_params=params(),
        name="group_columns",
    )(places, slab)


def group_rows(blocks, places, groups, share, widths):
    devices, keep, _ = blocks.shape
    unknowns = devices * share
    chunk = LANES - share
    steps = places.shape[0]
    per = devices // steps
    rows = unknowns // groups
    starts = [sum(widths[:i]) for i in range(len(widths))]
    outs = 4
    each = groups // outs

    def kernel(pos_ref, x_ref, *refs):
        out_refs, (extra, spread) = refs[:-2], refs[-2:]
        step = pl.program_id(0)

        @pl.when(step < steps)
        def _():
            for b in range(per):
                start = b * share
                for k in range(share // chunk):
                    extra[b * SUB:(b + 1) * SUB, chunk * k:chunk * (k + 1)] = x_ref[b, SUB * k:SUB * k + SUB, share:]
                for u in range(keep):
                    spread[pl.ds(pos_ref[0, 0, start + u], 1), :] = x_ref[b, u:u + 1, :]
                for u in range(SUB):
                    at = b * SUB + u
                    spread[pl.ds(pos_ref[0, 0, start + keep + u], 1), :] = extra[at:at + 1, :]

        @pl.when(step >= steps)
        def _():
            def turn(e, carry):
                g = (step - steps) * each + e
                for ref, start, width in zip(out_refs, starts, widths):
                    for k in range(width // LANES):
                        at = pl.multiple_of(g * rows + start + k * LANES, LANES)
                        ref[e, :, k * LANES:(k + 1) * LANES] = spread[pl.ds(at, LANES), :].T[:share]
                return carry

            lax.fori_loop(0, each, turn, 0)

    late = lambda g: (jnp.maximum(g - steps, 0), 0, 0)
    early = lambda g: (jnp.minimum(g, steps - 1), 0, 0)
    return pl.pallas_call(
        kernel,
        grid=(steps + outs,),
        in_specs=[
            pl.BlockSpec((1, 1, per * share), early, memory_space=pltpu.SMEM),
            pl.BlockSpec((per, keep, LANES), early),
        ],
        out_specs=[pl.BlockSpec((each, share, w), late) for w in widths],
        scratch_shapes=[
            pltpu.VMEM((per * SUB, LANES), jnp.float32),
            pltpu.VMEM((unknowns, LANES), jnp.float32),
        ],
        out_shape=[pltpu.HBM((groups, share, w), jnp.float32) for w in widths],
        compiler_params=params(),
        name="group_rows",
    )(places, blocks)


def tile_and_product(turned, v_hi, v_lo, where, tile, cols, share, offset):
    groups, _, rows = turned.shape
    span = rows // cols
    columns, width = v_hi.shape
    steps = 2
    wide = width // steps
    pairs = cols // 2

    def kernel(where_ref, x_ref, hi_ref, lo_ref, *refs):
        tile_ref, other_ref, mine_ref, x_in, x_hi, x_lo, held, x_sem, sem = refs[-9:]
        step = pl.program_id(0)
        store = pltpu.make_async_copy(held, tile_ref.at[:, offset:offset + span, :], sem)

        @pl.when(step == 0)
        def _():
            parts = [slice(k * LANES, (k + 1) * LANES) for k in range(rows // LANES)]
            fetches = [
                pltpu.make_async_copy(x_ref.at[:, :, p], x_in.at[:, :, p], x_sem.at[k]) for k, p in enumerate(parts)
            ]
            for fetch in fetches:
                fetch.start()
            for k in range(rows // LANES):
                fetches[k].wait()
                x = x_in[:, :, k * LANES:(k + 1) * LANES].reshape(columns, LANES).T
                hi = x.astype(jnp.bfloat16)
                x_hi[k * LANES:(k + 1) * LANES, :] = hi
                x_lo[k * LANES:(k + 1) * LANES, :] = (x - hi.astype(jnp.float32)).astype(jnp.bfloat16)
                for s in range(0, LANES, SUB):
                    c, m = divmod(k * LANES + s, span)
                    held[c, m:m + SUB, :] = x[s:s + SUB]
            store.start()

        part = (
            jnp.dot(x_hi[...], hi_ref[...], preferred_element_type=jnp.float32)
            + jnp.dot(x_hi[...], lo_ref[...], preferred_element_type=jnp.float32)
            + jnp.dot(x_lo[...], hi_ref[...], preferred_element_type=jnp.float32)
        )
        even = where_ref[0] == 0
        for c in range(pairs):
            slot = c ^ where_ref[1]
            first = part[2 * c * span:(2 * c + 1) * span]
            second = part[(2 * c + 1) * span:(2 * c + 2) * span]
            other_ref[slot] = jnp.where(even, second, first)
            mine_ref[slot] = jnp.where(even, first, second)

        @pl.when(step == steps - 1)
        def _():
            store.wait()

    half = jax.ShapeDtypeStruct((pairs, span, width), jnp.float32)
    half_spec = pl.BlockSpec((pairs, span, wide), lambda g, where: (0, 0, g))
    in_specs = [pl.BlockSpec(memory_space=pl.ANY)]
    in_specs += [pl.BlockSpec((columns, wide), lambda g, where: (0, g))] * 2
    operands = [where, turned, v_hi, v_lo]
    aliases = {}
    if tile is not None:
        aliases = {len(operands): 0}
        operands.append(tile)
        in_specs.append(pl.BlockSpec(memory_space=pl.ANY))
    return pl.pallas_call(
        kernel,
        grid_spec=pltpu.PrefetchScalarGridSpec(
            num_scalar_prefetch=1,
            grid=(steps,),
            in_specs=in_specs,
            out_specs=[pl.BlockSpec(memory_space=pl.ANY), half_spec, half_spec],
            scratch_shapes=[
                pltpu.VMEM((groups, share, rows), jnp.float32),
                pltpu.VMEM((rows, columns), jnp.bfloat16),
                pltpu.VMEM((rows, columns), jnp.bfloat16),
                pltpu.VMEM((cols, span, columns), jnp.float32),
                pltpu.SemaphoreType.DMA((rows // LANES,)),
                pltpu.SemaphoreType.DMA,
            ],
        ),
        out_shape=[jax.ShapeDtypeStruct((cols, share, columns), jnp.float32), half, half],
        input_output_aliases=aliases,
        compiler_params=params(),
        cost_estimate=pl.CostEstimate(flops=6 * rows * columns * width, bytes_accessed=8 * rows * columns, transcendentals=0),
    )(*operands)


def shards(normal_matrix, new_index, check_vectors):
    row_count = lax.axis_size("row")
    col_count = lax.axis_size("col")
    devices = row_count * col_count
    share, unknowns = normal_matrix.shape
    rows = unknowns // row_count
    steps = STEPS

    tile, lane = new_index // TILE, new_index % TILE
    within_col = tile // col_count * TILE + lane
    column_places = (within_col // share * col_count + tile % col_count) * share + within_col % share
    within_row = tile // row_count * TILE + lane
    owner, m = within_row // share, within_row % share
    spot = jnp.zeros_like(m)
    start = 0
    for span in SPANS:
        spot = jnp.where((m >= start) & (m < start + span), start * col_count + owner * span + m - start, spot)
        start += span
    row_places = tile % row_count * rows + spot
    column_places = column_places.reshape(steps, 1, unknowns // steps)
    row_places = row_places.reshape(steps, 1, unknowns // steps)

    along = lambda x: lax.all_to_all(x, "row", split_axis=0, concat_axis=0, tiled=True)
    flip = lambda x, bits: lax.ppermute(x, "col", [(i, i ^ bits) for i in range(col_count)])
    groups = [list(range(p, col_count, 2)) for p in range(2)]
    widths = [s * col_count for s in SPANS]

    in_hbm = lambda x: pltpu.with_memory_space_constraint(x, pltpu.HBM)
    outgoing = group_columns(in_hbm(normal_matrix), column_places, devices)
    arrived = lax.all_to_all(outgoing, ("row", "col"), split_axis=0, concat_axis=0, tiled=True)
    v_hi = lax.reduce_precision(check_vectors, 8, 7)
    v_lo = (check_vectors - v_hi).astype(jnp.bfloat16)
    v_hi = v_hi.astype(jnp.bfloat16)
    me = lax.axis_index("col").astype(jnp.int32)

    chosen = group_rows(arrived, row_places, row_count, share, widths)

    tile_layout = None
    sums = []
    last, held = arrived, None
    offset = 0
    for q, span in enumerate(SPANS):
        final = q == len(SPANS) - 1
        send, _ = lax.optimization_barrier((chosen[q], last))
        last = along(send)
        piece = last
        seat = me
        if held is not None:
            piece, _ = lax.optimization_barrier((last, held))
            seat, _ = lax.optimization_barrier((me, held))
        where = jnp.stack([seat % 2, jnp.zeros_like(seat) if final else seat // 2])
        tile_layout, other, mine = tile_and_product(
            piece, in_hbm(v_hi), in_hbm(v_lo), where, tile_layout, col_count, share, offset
        )
        offset += span
        theirs = flip(other, 1)
        if final:
            both = mine + theirs
            parts = lax.all_to_all(both, "col", split_axis=0, concat_axis=0, axis_index_groups=groups, tiled=True)
            sums.append(parts.sum(axis=0))
        else:
            both = [mine[i:i + 2] + theirs[i:i + 2] for i in range(0, col_count // 2, 2)]
            both = lax.optimization_barrier(tuple(both))
            near = both[0]
            for y in range(1, col_count // 4):
                got = flip(both[y], 4 * y)
                near = near + got
            held = tuple(both[1:])
            got = flip(near[1], 2)
            sums.append(near[0] + got)
    return tile_layout.reshape(rows, unknowns // col_count), jnp.concatenate(sums, axis=0)


def solution(mesh):
    return jax.shard_map(
        shards,
        mesh=mesh,
        in_specs=(P(("row", "col"), None), P(), P("col", None)),
        out_specs=(P("row", "col"), P(("row", "col"), None)),
        check_vma=False,
    )
```
